32 devices in a mesh: parts: 2 (over y), group: 2 (over x), dev: 4 (over z), pair: 2 (over core).
Axes of the slice: x: 2, y: 2, z: 4, core: 2. Of those that a mesh axis runs over, the one named last changes fastest.
Arguments:
- tokens: bfloat16 [2048, 2048], P(('parts', 'group', 'dev', 'pair')), parts along dimension 0, may hold values from -6 to 6
- expert_ids: int32 [2048, 2], P(('parts', 'group', 'dev', 'pair')), parts along dimension 0, may hold values from 0 to 3, all different within a row; in each aligned block of 64 rows (0 to 63, 64 to 127, ...) at most 48 rows name the same one
- route_scores: float32 [2048, 2], P(('parts', 'group', 'dev', 'pair')), parts along dimension 0, may hold values from 0.05 to 1
- w_gate: bfloat16 [8, 2048, 384], P(('group', 'dev'), None, 'pair'), may hold values from -0.125 to 0.125
- w_up: bfloat16 [8, 2048, 384], P(('group', 'dev'), None, 'pair'), may hold values from -0.125 to 0.125
- w_down: bfloat16 [8, 2048, 384], P(('group', 'dev'), None, 'pair'), may hold values from -0.21875 to 0.21875
Outputs:
- mixed_out: bfloat16 [2048, 2048], P(('parts', 'group', 'dev', 'pair')), parts along dimension 0
The draws below stay inside these ranges and needn't reach their ends.
There are 2 independent parts, one for each index of `parts`. The reference program is written for one: setup_inputs(seed, part) draws one part's arguments, and reference() takes and returns one part's arrays. A program takes and returns all parts, laid end to end along the dimension named above; an argument that names none is the same for every part. Nothing has to cross between parts.
Inputs may be any that keep to these rules, and one draw needn't show every extreme that they name: `expert_ids`: each row names 2 different experts. Within each aligned block of 64 rows (the tokens of one device) no expert is named more than 48 times, a bound that some block reaches.
All inputs are finite; a program needn't handle non-finite values.
Results may differ from the reference program's by a relative error of at most 0.0057.
Values may be sent and summed in bfloat16 or wider, within the bound.
No kernel may reach another device: no remote copies, remote signals or barrier semaphores. Data moves between devices by JAX's collectives and lax.ppermute only.
A program may use at most 128 MiB of HBM per device.

```python
import math
import jax
import jax.numpy as jnp
import numpy as np
from jax import lax

D = 2048
HID = 768
TOK_DEV = 64
EXPERTS = 4
TOP = 2
CAP = 48
TOKENS = 1024
N_GROUP = 2
N_DEV = 4
N_PAIR = 2


def block_levels(stream_key, extent, split, low, top_value):
    level = 1.0
    for position, parts in split:
        draws = jax.random.uniform(jax.random.fold_in(jax.random.fold_in(stream_key, 6), position), (parts,), jnp.float32, low / len(split), top_value / len(split))
        level = level * jnp.repeat(jnp.exp(draws), extent[position] // parts).reshape((-1,) + (1,) * (len(extent) - 1 - position))
    return level


def shared_out(stream_key, own, number, rows, number_of, top, reach, skew):
    order = jax.random.permutation(stream_key, number_of)
    heavy_load, ordinary = load_shares(number_of, rows * top, reach, skew, True), load_shares(number_of, rows * top, reach, skew, False)
    places = jnp.arange(number_of)

    def named(tallies, offset_by):
        used = int((tallies > 0).sum())
        fixed = max(1, used // 4)
        moved = fixed + (places - fixed + offset_by * (used - fixed)) % max(1, number_of - fixed)
        return jnp.zeros((number_of,), jnp.int32).at[order[jnp.where(places < fixed, places, moved)]].set(jnp.asarray(tallies, jnp.int32))

    tallies = jnp.where(number % 4 == 0, named(heavy_load, number // 4), named(ordinary, number - number // 4 - 1))
    mixed = jax.random.permutation(jax.random.fold_in(own, 3), number_of)
    giver, taker = mixed[0:number_of // 2 * 2:2], mixed[1:number_of // 2 * 2:2]
    margin = jnp.minimum(tallies[giver] - 1, reach - tallies[taker]) // 2
    margin = jnp.where((giver == order[0]) | (taker == order[0]) | (tallies[taker] == 0), 0, jnp.maximum(margin, 0))
    moved = jax.random.randint(jax.random.fold_in(own, 4), (number_of // 2,), 0, 1 << 20) % (margin + 1)
    tallies = tallies.at[giver].add(-moved).at[taker].add(moved)
    labels = jnp.searchsorted(jnp.cumsum(tallies), jnp.arange(rows * top), side="right").astype(jnp.int32)
    listing = labels.reshape(top, rows).T
    listing = listing[jax.random.permutation(jax.random.fold_in(own, 1), rows)]
    offset_by = jax.random.randint(jax.random.fold_in(own, 2), (rows, 1), 0, top)
    return jnp.take_along_axis(listing, (jnp.arange(top)[None, :] + offset_by) % top, axis=1)


def load_shares(number_of, total, bound, slope, full):
    weights = [(1 << 20) // math.isqrt(rank ** slope) + 1 for rank in range(1, number_of + 1)]
    largest = bound if full else min(bound, max(-(-total // number_of), total * weights[0] // sum(weights)))
    least = 1 if total - largest >= number_of - 1 else 0
    counts, rest = [largest] + [least] * (number_of - 1), total - largest - least * (number_of - 1)
    while rest > 0:
        movable = [i for i in range(1, number_of) if counts[i] < largest] or [i for i in range(1, number_of) if counts[i] < bound]
        mass, left = sum([weights[i] for i in movable]), rest
        for i in movable:
            more = min(bound - counts[i], max(1, left * weights[i] // mass), rest)
            counts[i] = counts[i] + more
            rest = rest - more
    return np.array(counts)


def scatter_about(key, dims, deviation, most, pieces=(), kind=jnp.bfloat16):
    drawn = jax.random.normal(key, dims, jnp.float32) * deviation
    if len(pieces) > 0:
        drawn = block_levels(key, dims, pieces, -0.22, 0.18) * drawn
    return jnp.clip(drawn, min=-most, max=most).astype(kind)


def setup_inputs(seed: int = 0, part: int = 0) -> dict:
    keys = jax.random.split(jax.random.key(seed), 7)
    part_splits = jax.random.split(jax.random.fold_in(keys[6], part), 7)
    tokens = scatter_about(part_splits[0], (TOKENS, D), 1.0, 6.0, ((0, 16),))
    expert_ids_keys = jax.random.split(jax.random.fold_in(part_splits[1], 1), TOKENS // TOK_DEV)
    expert_ids_turns = jax.random.permutation(jax.random.fold_in(part_splits[1], 3), TOKENS // TOK_DEV)
    expert_ids = jax.vmap(lambda own, number: shared_out(jax.random.fold_in(part_splits[1], 2), own, number, TOK_DEV, EXPERTS, TOP, CAP, 2))(expert_ids_keys, expert_ids_turns).reshape((TOKENS, TOP))
    route_scores = jnp.clip(jnp.exp(math.log(1.0) - 2.9957323 * jax.random.uniform(part_splits[2], (TOKENS, TOP), jnp.float32) ** block_levels(part_splits[2], (TOKENS, TOP), ((0, 16),), -0.2, 0.2)), 0.05, 1.0)
    w_gate = scatter_about(keys[3], (2 * EXPERTS, D, HID // 2), D ** -0.5, 0.125, ((0, 8), (2, 2)))
    w_up = scatter_about(keys[4], (2 * EXPERTS, D, HID // 2), D ** -0.5, 0.125, ((0, 8), (2, 2)))
    w_down = scatter_about(keys[5], (2 * EXPERTS, D, HID // 2), HID ** -0.5, 0.21875, ((0, 8), (2, 2)))
    return dict(tokens=tokens, expert_ids=expert_ids, route_scores=route_scores, w_gate=w_gate, w_up=w_up, w_down=w_down)


def joined(weights):
    return weights.reshape(EXPERTS, 2, D, HID // 2).transpose(0, 2, 1, 3).reshape(EXPERTS, D, HID)


def reference(tokens, expert_ids, route_scores, w_gate, w_up, w_down):
    route_weight = route_scores / jnp.sum(route_scores, axis=1, keepdims=True)
    row_limit = N_GROUP * N_DEV * N_PAIR * CAP
    gate_all = joined(w_gate)
    up_all = joined(w_up)
    down_all = joined(w_down)

    def per_expert(running, stacked):
        gate_one, up_one, down_one, expert = stacked
        matches = expert_ids == expert
        weighting = jnp.sum(jnp.where(matches, route_weight, 0.0), axis=1)
        chosen = jnp.any(matches, axis=1)
        row_index = jnp.nonzero(chosen, size=row_limit, fill_value=0)[0].astype(jnp.int32)
        filled = jnp.arange(row_limit, dtype=jnp.int32) < jnp.sum(chosen.astype(jnp.int32))
        gathered = tokens[row_index]
        gate_act = jnp.dot(gathered, gate_one, preferred_element_type=jnp.float32)
        up_act = jnp.dot(gathered, up_one, preferred_element_type=jnp.float32)
        hidden = (jax.nn.silu(gate_act) * up_act).astype(jnp.bfloat16)
        output = lax.dot_general(hidden, down_one, (((1,), (1,)), ((), ())), preferred_element_type=jnp.float32).astype(jnp.bfloat16)
        weight = jnp.where(filled, weighting[row_index], 0.0)
        running = running.at[row_index].add(weight[:, None] * output.astype(jnp.float32))
        return running, None

    start = jnp.zeros((TOKENS, D), jnp.float32)
    running, _ = lax.scan(per_expert, start, (gate_all, up_all, down_all, jnp.arange(EXPERTS, dtype=jnp.int32)))
    return running.astype(jnp.bfloat16)
```

```python
import functools

import jax
import jax.numpy as jnp
from jax import lax
from jax.experimental import pallas as pl
from jax.experimental.pallas import tpu as pltpu
from jax.sharding import PartitionSpec as P

CHIPS = ("group", "dev")
LANES = 128
F32, BF16 = jnp.float32, jnp.bfloat16


def partner_2(x, axis, apart):
    return lax.ppermute(x, axis, [(i, i ^ 1 << apart) for i in range(lax.axis_size(axis))])


def expert_block(batch_rows, gate_piece, up_piece, down_piece):
    gate_act = jnp.dot(batch_rows, gate_piece, preferred_element_type=jnp.float32)
    up_act = jnp.dot(batch_rows, up_piece, preferred_element_type=jnp.float32)
    hidden = (jax.nn.silu(gate_act) * up_act).astype(jnp.bfloat16)
    return lax.dot_general(
        hidden, down_piece, (((1,), (1,)), ((), ())), preferred_element_type=jnp.float32
    )


def expert_capacity(rows_dev, top_count, experts):
    return 2 * max(1, 3 * rows_dev * top_count // (4 * experts))


def gathered_weights(tokens, expert_ids, route_scores, w_gate, w_up, w_down):
    rows_dev, features = tokens.shape
    top_count = expert_ids.shape[1]
    dest_count = lax.axis_size(("group", "dev"))
    experts = dest_count // 2
    half_cap = expert_capacity(rows_dev, top_count, experts) // 2
    route_weight = route_scores / jnp.sum(route_scores, axis=1, keepdims=True)
    flat_ids = expert_ids.reshape(-1)
    onehot = (flat_ids[:, None] == jnp.arange(experts, dtype=jnp.int32)[None, :]).astype(jnp.int32)
    before = jnp.cumsum(onehot, axis=0) - onehot
    rank_in = jnp.sum(before * onehot, axis=1)
    target = 2 * flat_ids + rank_in // half_cap
    position = target * half_cap + rank_in % half_cap
    owners = jnp.arange(rows_dev * top_count, dtype=jnp.int32) // top_count
    outgoing = (
        jnp.zeros((dest_count * half_cap, features), jnp.bfloat16).at[position].set(tokens[owners])
    )
    outgoing = outgoing.reshape(dest_count, half_cap, features)
    arrived = lax.all_to_all(outgoing, ("group", "dev"), split_axis=0, concat_axis=0, tiled=True)
    batch_rows = arrived.reshape(dest_count * half_cap, features)
    partner = partner_2((w_gate[0], w_up[0], w_down[0]), "dev", 0)
    gate_half = jnp.concatenate([w_gate[0], partner[0]], axis=1)
    up_half = jnp.concatenate([w_up[0], partner[1]], axis=1)
    down_half = jnp.concatenate([w_down[0], partner[2]], axis=1)
    full_gate, full_up, full_down = (
        lax.all_gather(gate_half, "pair", axis=1, tiled=True),
        lax.all_gather(up_half, "pair", axis=1, tiled=True),
        lax.all_gather(down_half, "pair", axis=1, tiled=True),
    )
    result = expert_block(batch_rows, full_gate, full_up, full_down)
    answer = result.astype(jnp.bfloat16).reshape(dest_count, half_cap, features)
    returned = lax.all_to_all(answer, ("group", "dev"), split_axis=0, concat_axis=0, tiled=True)
    picked = returned.reshape(dest_count * half_cap, features)[position].astype(jnp.float32)
    weighted = picked * route_weight.reshape(-1)[:, None]
    mixed_out = jnp.sum(weighted.reshape(rows_dev, top_count, features), axis=1)
    return mixed_out.astype(jnp.bfloat16)


def swap(x, mask):
    return lax.ppermute(x, CHIPS, [(i, i ^ mask) for i in range(lax.axis_size(CHIPS))])


def iota(shape, dim):
    return lax.broadcasted_iota(jnp.int32, shape, dim)


def coefficient(meta, expert, experts):
    lane = iota(meta.shape, 1)
    hit = (lane == expert) | (lane == expert + experts) | (lane == expert + 2 * experts)
    return jnp.sum(jnp.where(hit, meta.astype(F32), 0.0), axis=1, keepdims=True)


def places(coef):
    rows = coef.shape[0]
    chosen = jnp.broadcast_to(jnp.where(coef > 0.0, 1.0, 0.0), (rows, rows))
    here, there = iota((rows, rows), 0), iota((rows, rows), 1)
    chosen_row = jnp.sum(jnp.where(here == there, chosen, 0.0), axis=0, keepdims=True)
    rank_row = jnp.sum(jnp.where(here < there, chosen, 0.0), axis=0, keepdims=True)
    return chosen_row, rank_row


def packed(block, coef, cap):
    rows = coef.shape[0]
    chosen_row, rank_row = places(coef)
    slot = iota((cap, rows), 0).astype(F32)
    select = jnp.where((slot == rank_row) & (chosen_row > 0.0), 1.0, 0.0).astype(BF16)
    return jnp.dot(select, block, preferred_element_type=F32).astype(BF16)


def unpacked(part, coef):
    rows, cap = coef.shape[0], part.shape[0]
    chosen_row, _ = places(coef)
    here, there = iota((rows, rows), 0), iota((rows, rows), 1)
    rank = jnp.sum(jnp.where(there < here, chosen_row, 0.0), axis=1, keepdims=True)
    slot = iota((rows, cap), 1).astype(F32)
    select = jnp.where((slot == rank) & (coef > 0.0), 1.0, 0.0).astype(BF16)
    return coef * jnp.dot(select, part, preferred_element_type=F32)


def prepare_kernel(experts, cap, who, tokens, ids, scores, ext, side, far):
    rows, features = tokens.shape
    weight = scores[...] / jnp.sum(scores[...], axis=1, keepdims=True)
    lane = iota((rows, LANES), 1)
    meta = jnp.zeros((rows, LANES), F32)
    for k in range(ids.shape[1]):
        rest = weight[:, k : k + 1]
        for part in range(3):
            term = rest.astype(BF16).astype(F32)
            meta += jnp.where(lane == ids[:, k : k + 1] + part * experts, term, 0.0)
            rest = rest - term
    ext[:, :features] = tokens[...]
    ext[:, features:] = meta.astype(BF16)
    side[...] = packed(tokens[...], coefficient(meta, who[1], experts), cap)
    far[...] = packed(tokens[...], coefficient(meta, who[2], experts), cap)


def pack_kernel(experts, cap, who, block, side):
    features = side.shape[1]
    coef = coefficient(block[:, features:], who[1], experts)
    side[...] = packed(block[:, :features], coef, cap)


def expert_kernel(experts, whole, who, *refs):
    weights, blocks = refs[:6], refs[6 : 6 + (len(refs) - 6) // 2]
    outs = refs[6 + len(blocks) :]
    features = outs[0].shape[1]
    rows = jnp.concatenate([b[:, :features] for b in blocks], axis=0)
    total = None
    for gate, up, down in (weights[:3], weights[3:]):
        across = (((1,), (1,)), ((), ()))
        gate_act = lax.dot_general(rows, gate[...], across, preferred_element_type=F32)
        up_act = lax.dot_general(rows, up[...], across, preferred_element_type=F32)
        hidden = (gate_act / (1.0 + jnp.exp(-gate_act)) * up_act).astype(BF16)
        part = jnp.dot(hidden, down[...], preferred_element_type=F32)
        total = part if total is None else total + part
    at = 0
    for i, (block, out) in enumerate(zip(blocks, outs)):
        part = total[at : at + block.shape[0]]
        if i < whole:
            part = part * coefficient(block[:, features:], who[0], experts)
        out[...] = part.astype(out.dtype)
        at += block.shape[0]


def join_kernel(experts, slots, who, block, share, *refs):
    out, backs, sums = refs[-1], refs[: len(slots)], refs[len(slots) : -1]
    features = share.shape[1]
    total = share[...].astype(F32)
    for slot, back in zip(slots, backs):
        total += unpacked(back[...], coefficient(block[:, features:], who[slot], experts))
    for other in sums:
        total += other[...].astype(F32)
    out[...] = total.astype(out.dtype)


def call(kernel, name, who, operands, outs, flops=0):
    shapes = [jax.ShapeDtypeStruct(s, d) for s, d in outs]
    moved = sum(a.size * a.dtype.itemsize for a in operands) + sum(
        s.size * s.dtype.itemsize for s in shapes
    )
    result = pl.pallas_call(
        kernel,
        out_shape=shapes,
        in_specs=[pl.BlockSpec(memory_space=pltpu.SMEM)]
        + [pl.BlockSpec(memory_space=pltpu.VMEM)] * len(operands),
        out_specs=[pl.BlockSpec(memory_space=pltpu.VMEM)] * len(shapes),
        compiler_params=pltpu.CompilerParams(vmem_limit_bytes=32 << 20),
        cost_estimate=pl.CostEstimate(flops=flops, bytes_accessed=moved, transcendentals=0),
        name=name,
    )(who, *operands)
    return result[0] if len(shapes) == 1 else result


def travelling_tokens(tokens, expert_ids, route_scores, w_gate, w_up, w_down):
    rows, features = tokens.shape
    groups, devs = lax.axis_size("group"), lax.axis_size("dev")
    experts = groups * devs // 2
    cap = min(rows, expert_capacity(rows, expert_ids.shape[1], experts))
    near, mid, cross = 1, devs // 2, devs
    group, half = lax.axis_index("group"), lax.axis_index("dev") // 2
    per_group = devs // 2
    own_expert = group * per_group + half
    side_expert = (1 - group) * per_group + half
    far_expert = (1 - group) * per_group + (per_group - 1 - half)
    who = jnp.stack([own_expert, side_expert, far_expert]).astype(jnp.int32)

    mine = tuple(w[0].T for w in (w_gate, w_up, w_down))
    pairs = [(i, lax.axis_size("pair") - 1 - i) for i in range(lax.axis_size("pair"))]
    theirs = tuple(lax.ppermute(w, "pair", pairs) for w in mine)
    weights = mine + theirs
    width = features + LANES
    per_row = 2 * 3 * 2 * mine[0].shape[0] * features

    def packing(block):
        kernel = functools.partial(pack_kernel, experts, cap)
        return call(kernel, "pack", who, (block,), [((cap, features), BF16)], 2 * cap * rows * features)

    def compute(name, blocks, outs):
        whole = sum(b.shape[1] == width for b in blocks)
        kernel = functools.partial(expert_kernel, experts, whole)
        shapes = [((b.shape[0], features), d) for b, d in zip(blocks, outs)]
        flops = per_row * sum(b.shape[0] for b in blocks)
        return call(kernel, name, who, weights + tuple(blocks), shapes, flops)

    def join(block, share, slots, backs, sums):
        kernel = functools.partial(join_kernel, experts, slots)
        operands = (block, share) + tuple(backs) + tuple(sums)
        return call(kernel, "join", who, operands, [((rows, features), BF16)], 2 * rows * cap * features)

    ext, side_0, far_0 = call(
        functools.partial(prepare_kernel, experts, cap),
        "prepare",
        who,
        (tokens, expert_ids, route_scores),
        [((rows, width), BF16), ((cap, features), BF16), ((cap, features), BF16)],
        4 * cap * rows * features,
    )
    block_2 = swap(ext, mid)
    block_1 = swap(ext, near)
    rows_0 = swap(side_0, cross)
    rows_far = swap(far_0, cross + mid + near)
    block_3 = swap(block_2, near)
    rows_1 = swap(packing(block_1), cross)
    rows_2 = swap(packing(block_2), cross)

    share_0, share_1, back_0 = compute("experts_0", (ext, block_1, rows_0), (F32, F32, BF16))
    share_2, back_1 = compute("experts_1", (block_2, rows_1), (F32, BF16))
    share_3 = compute("experts_2", (block_3,), (BF16,))
    back_2, back_far = compute("experts_3", (rows_2, rows_far), (BF16, BF16))

    from_3 = swap(share_3, near)
    back_0, back_1, back_2 = swap(back_0, cross), swap(back_1, cross), swap(back_2, cross)
    back_far = swap(back_far, cross + mid + near)
    from_1 = swap(join(block_1, share_1, (1,), (back_1,), ()), near)
    from_2 = swap(join(block_2, share_2, (1,), (back_2,), (from_3,)), mid)
    return join(ext, share_0, (1, 2), (back_0, back_far), (from_1, from_2))


def shards(*args):
    cube = lax.axis_size("group") == 2 and lax.axis_size("dev") == 4 and lax.axis_size("pair") == 2
    return (travelling_tokens if cube else gathered_weights)(*args)


def solution(mesh):
    in_specs = (
        P(("parts", "group", "dev", "pair"), None),
        P(("parts", "group", "dev", "pair"), None),
        P(("parts", "group", "dev", "pair"), None),
        P(("group", "dev"), None, "pair"),
        P(("group", "dev"), None, "pair"),
        P(("group", "dev"), None, "pair"),
    )
    out_specs = P(("parts", "group", "dev", "pair"), None)
    return jax.shard_map(shards, mesh=mesh, in_specs=in_specs, out_specs=out_specs, check_vma=False)
```

```python
import functools

import jax
import jax.numpy as jnp
from jax import lax
from jax.experimental import pallas as pl
from jax.experimental.pallas import tpu as pltpu
from jax.sharding import PartitionSpec as P


CHIPS = ("group", "dev")
LANES = 128
VMEM_LIMIT = 12 << 20
F32, BF16 = jnp.float32, jnp.bfloat16
LAG = 800


def partner_2(x, axis, apart):
    return lax.ppermute(x, axis, [(i, i ^ 1 << apart) for i in range(lax.axis_size(axis))])


def expert_block(batch_rows, gate_piece, up_piece, down_piece):
    gate_act = jnp.dot(batch_rows, gate_piece, preferred_element_type=jnp.float32)
    up_act = jnp.dot(batch_rows, up_piece, preferred_element_type=jnp.float32)
    hidden = (jax.nn.silu(gate_act) * up_act).astype(jnp.bfloat16)
    return lax.dot_general(
        hidden, down_piece, (((1,), (1,)), ((), ())), preferred_element_type=jnp.float32
    )


def expert_capacity(rows_dev, top_count, experts):
    return 2 * max(1, 3 * rows_dev * top_count // (4 * experts))


def gathered_weights(tokens, expert_ids, route_scores, w_gate, w_up, w_down):
    rows_dev, features = tokens.shape
    top_count = expert_ids.shape[1]
    dest_count = lax.axis_size(("group", "dev"))
    experts = dest_count // 2
    half_cap = expert_capacity(rows_dev, top_count, experts) // 2
    route_weight = route_scores / jnp.sum(route_scores, axis=1, keepdims=True)
    flat_ids = expert_ids.reshape(-1)
    onehot = (flat_ids[:, None] == jnp.arange(experts, dtype=jnp.int32)[None, :]).astype(jnp.int32)
    before = jnp.cumsum(onehot, axis=0) - onehot
    rank_in = jnp.sum(before * onehot, axis=1)
    target = 2 * flat_ids + rank_in // half_cap
    position = target * half_cap + rank_in % half_cap
    owners = jnp.arange(rows_dev * top_count, dtype=jnp.int32) // top_count
    outgoing = (
        jnp.zeros((dest_count * half_cap, features), jnp.bfloat16).at[position].set(tokens[owners])
    )
    outgoing = outgoing.reshape(dest_count, half_cap, features)
    arrived = lax.all_to_all(outgoing, ("group", "dev"), split_axis=0, concat_axis=0, tiled=True)
    batch_rows = arrived.reshape(dest_count * half_cap, features)
    partner = partner_2((w_gate[0], w_up[0], w_down[0]), "dev", 0)
    gate_half = jnp.concatenate([w_gate[0], partner[0]], axis=1)
    up_half = jnp.concatenate([w_up[0], partner[1]], axis=1)
    down_half = jnp.concatenate([w_down[0], partner[2]], axis=1)
    full_gate, full_up, full_down = (
        lax.all_gather(gate_half, "pair", axis=1, tiled=True),
        lax.all_gather(up_half, "pair", axis=1, tiled=True),
        lax.all_gather(down_half, "pair", axis=1, tiled=True),
    )
    result = expert_block(batch_rows, full_gate, full_up, full_down)
    answer = result.astype(jnp.bfloat16).reshape(dest_count, half_cap, features)
    returned = lax.all_to_all(answer, ("group", "dev"), split_axis=0, concat_axis=0, tiled=True)
    picked = returned.reshape(dest_count * half_cap, features)[position].astype(jnp.float32)
    weighted = picked * route_weight.reshape(-1)[:, None]
    mixed_out = jnp.sum(weighted.reshape(rows_dev, top_count, features), axis=1)
    return mixed_out.astype(jnp.bfloat16)


def swap(x, mask):
    return lax.ppermute(x, CHIPS, [(i, i ^ mask) for i in range(lax.axis_size(CHIPS))])


def iota(shape, dim):
    return lax.broadcasted_iota(jnp.int32, shape, dim)


def expert_of(slot, experts):
    group, half = lax.axis_index("group"), lax.axis_index("dev") // 2
    per_group = experts // lax.axis_size("group")
    group = group if slot == 0 else 1 - group
    return group * per_group + (per_group - 1 - half if slot == 2 else half)


def coefficient(meta, expert, experts):
    lane = iota(meta.shape, 1)
    hit = (lane == expert) | (lane == expert + experts) | (lane == expert + 2 * experts)
    return jnp.sum(jnp.where(hit, meta.astype(F32), 0.0), axis=1, keepdims=True)


def places(coef):
    rows = coef.shape[0]
    chosen = jnp.broadcast_to(jnp.where(coef > 0.0, 1.0, 0.0), (rows, rows))
    here, there = iota((rows, rows), 0), iota((rows, rows), 1)
    chosen_row = jnp.sum(jnp.where(here == there, chosen, 0.0), axis=0, keepdims=True)
    rank_row = jnp.sum(jnp.where(here < there, chosen, 0.0), axis=0, keepdims=True)
    return chosen_row, rank_row


def packed(block, coef, cap):
    rows = coef.shape[0]
    chosen_row, rank_row = places(coef)
    slot = iota((cap, rows), 0).astype(F32)
    select = jnp.where((slot == rank_row) & (chosen_row > 0.0), 1.0, 0.0).astype(BF16)
    return jnp.dot(select, block, preferred_element_type=F32).astype(BF16)


def unpacked(part, coef):
    rows, cap = coef.shape[0], part.shape[0]
    chosen_row, _ = places(coef)
    here, there = iota((rows, rows), 0), iota((rows, rows), 1)
    rank = jnp.sum(jnp.where(there < here, chosen_row, 0.0), axis=1, keepdims=True)
    slot = iota((rows, cap), 1).astype(F32)
    select = jnp.where((slot == rank) & (coef > 0.0), 1.0, 0.0).astype(BF16)
    return coef * jnp.dot(select, part, preferred_element_type=F32)


def column(row, rows):
    same = iota((rows, rows), 0) == iota((rows, rows), 1)
    return jnp.sum(jnp.where(same, jnp.broadcast_to(row, (rows, rows)), 0.0), axis=1, keepdims=True)


def prepare_kernel(experts, cap, tokens, ids, scores, ext, side, far, ids_here, scores_here, count, sems):
    rows, features = tokens.shape
    copies = [
        pltpu.make_async_copy(ids, ids_here, sems.at[0]),
        pltpu.make_async_copy(scores, scores_here, sems.at[1]),
        pltpu.make_async_copy(tokens, ext.at[:, :features], sems.at[2]),
    ]
    for copy in copies:
        copy.start()
    copies[0].wait()
    copies[1].wait()
    weight = scores_here[...] / jnp.sum(scores_here[...], axis=0, keepdims=True)
    lane = iota((rows, LANES), 1).astype(F32)
    meta = jnp.zeros((rows, LANES), F32)
    for k in range(ids.shape[0]):
        chosen = column(ids_here[k : k + 1, :].astype(F32), rows)
        rest = column(weight[k : k + 1, :], rows)
        for part in range(3):
            term = rest.astype(BF16).astype(F32)
            meta += jnp.where(lane == chosen + float(part * experts), term, 0.0)
            rest = rest - term
    ext[:, features:] = meta.astype(BF16)
    copies[2].wait()
    count[0] = 0

    @pl.loop(0, LAG * lax.axis_index("pair"))
    def _(i):
        count[0] = count[0] * 3 + i

    side[...] = packed(ext[:, :features], coefficient(meta, expert_of(1, experts), experts), cap)
    far[...] = packed(ext[:, :features], coefficient(meta, expert_of(2, experts), experts), cap)


def forward_kernel(experts, block_2, block_1, pass_3, side_2, side_1):
    features = pass_3.shape[1]
    for block, slot, out in ((block_2, 0, pass_3), (block_2, 1, side_2), (block_1, 1, side_1)):
        coef = coefficient(block[:, features:], expert_of(slot, experts), experts)
        out[...] = packed(block[:, :features], coef, out.shape[0])


def hold_kernel(*refs):
    half = len(refs) // 2
    copies = [
        pltpu.make_async_copy(src, dst, refs[-1].at[i])
        for i, (src, dst) in enumerate(zip(refs[:half], refs[half:]))
    ]
    for copy in copies:
        copy.start()
    for copy in copies:
        copy.wait()


def expert_kernel(experts, whole, packs, *refs):
    weights, blocks = refs[:6], refs[6 : 6 + whole + packs]
    outs = refs[6 + whole + packs :]
    features = outs[0].shape[1]
    rows = jnp.concatenate([b[:, :features] for b in blocks], axis=0)
    total = None
    for gate, up, down in (weights[:3], weights[3:]):
        across = (((1,), (1,)), ((), ()))
        gate_act = lax.dot_general(rows, gate[...], across, preferred_element_type=F32)
        up_act = lax.dot_general(rows, up[...], across, preferred_element_type=F32)
        hidden = (gate_act / (1.0 + jnp.exp(-gate_act)) * up_act).astype(BF16)
        part = jnp.dot(hidden, down[...], preferred_element_type=F32)
        total = part if total is None else total + part
    at = 0
    for i, (block, out) in enumerate(zip(blocks, outs)):
        part = total[at : at + block.shape[0]]
        if i < whole:
            part = part * coefficient(block[:, features:], expert_of(0, experts), experts)
        out[...] = part.astype(out.dtype)
        at += block.shape[0]


def join_kernel(experts, slots, block, share, *refs):
    out, features = refs[-1], share.shape[1]
    total = share[...].astype(F32)
    for slot, back in zip(slots, refs[:-1]):
        coef = coefficient(block[:, features:], expert_of(slot, experts), experts)
        total += unpacked(back[...], coef)
    out[...] = total.astype(out.dtype)


def add_kernel(share, one, two, out):
    out[...] = (share[...] + one[...].astype(F32) + two[...].astype(F32)).astype(out.dtype)


def call(kernel, operands, outs, flops=0, space=pltpu.VMEM, scratch=()):
    shapes = [jax.ShapeDtypeStruct(s, d) for s, d in outs]
    moved = sum(a.size * a.dtype.itemsize for a in (*operands, *shapes))
    if space is pltpu.HBM:
        operands = [pltpu.with_memory_space_constraint(a, space) for a in operands]
    result = pl.pallas_call(
        kernel,
        out_shape=shapes,
        in_specs=[pl.BlockSpec(memory_space=space)] * len(operands),
        out_specs=[pl.BlockSpec(memory_space=pltpu.VMEM)] * len(shapes),
        scratch_shapes=scratch,
        compiler_params=pltpu.CompilerParams(vmem_limit_bytes=VMEM_LIMIT),
        cost_estimate=pl.CostEstimate(flops=flops, bytes_accessed=moved, transcendentals=0),
    )(*operands)
    return result[0] if len(shapes) == 1 else result


def travelling_tokens(tokens, expert_ids, route_scores, w_gate, w_up, w_down):
    rows, features = tokens.shape
    top = expert_ids.shape[1]
    devs = lax.axis_size("dev")
    experts = lax.axis_size(CHIPS) // 2
    cap = min(rows, expert_capacity(rows, top, experts))
    near, mid, cross = 1, devs // 2, devs
    width = features + LANES

    mine = tuple(w[0].T for w in (w_gate, w_up, w_down))
    pair = lax.axis_size("pair")
    theirs = tuple(lax.ppermute(w, "pair", [(i, pair - 1 - i) for i in range(pair)]) for w in mine)
    shapes = [(w.shape, w.dtype) for w in mine]
    sems = [pltpu.SemaphoreType.DMA((len(mine),))]
    held = call(hold_kernel, mine, shapes, 0, pltpu.HBM, sems)
    weights = tuple(held) + theirs
    per_row = 2 * 3 * 2 * mine[0].shape[0] * features

    def compute(blocks, outs):
        whole = sum(b.shape[1] == width for b in blocks)
        kernel = functools.partial(expert_kernel, experts, whole, len(blocks) - whole)
        sizes = [b.shape[0] for b in blocks]
        shapes = [((n, features), d) for n, d in zip(sizes, outs)]
        return call(kernel, weights + tuple(blocks), shapes, per_row * sum(sizes))

    def join(block, share, backs, dtype=BF16):
        kernel = functools.partial(join_kernel, experts, tuple(slot for slot, _ in backs))
        operands = (block, share) + tuple(back for _, back in backs)
        return call(kernel, operands, [((rows, features), dtype)], 2 * rows * cap * features)

    packed_out = ((cap, features), BF16)
    scratch = [pltpu.VMEM((top, rows), jnp.int32), pltpu.VMEM((top, rows), F32)]
    scratch += [pltpu.SMEM((1,), jnp.int32), pltpu.SemaphoreType.DMA((3,))]
    ext, side_0, far_0 = call(
        functools.partial(prepare_kernel, experts, cap),
        (tokens, expert_ids.T, route_scores.T),
        [((rows, width), BF16), packed_out, packed_out],
        4 * cap * rows * features,
        pltpu.HBM,
        scratch,
    )
    block_2 = swap(ext, mid)
    block_1 = swap(ext, near)
    rows_0 = swap(side_0, cross)
    pass_3, side_2, side_1 = call(
        functools.partial(forward_kernel, experts),
        (block_2, block_1),
        [packed_out] * 3,
        6 * cap * rows * features,
    )
    rows_3 = swap(pass_3, near)
    rows_2 = swap(side_2, cross)
    rows_1 = swap(side_1, cross)
    rows_far = swap(far_0, cross + mid + near)

    share_0, share_1, share_2, back_0 = compute(
        (ext, block_1, block_2, rows_0), (F32, F32, F32, BF16)
    )
    back_3, back_2 = compute((rows_3, rows_2), (BF16, BF16))
    back_1, back_far = compute((rows_1, rows_far), (BF16, BF16))

    back_3 = swap(back_3, near)
    back_2 = swap(back_2, cross)
    back_1 = swap(back_1, cross)
    back_far = swap(back_far, cross + mid + near)
    back_0 = swap(back_0, cross)
    from_2 = swap(join(block_2, share_2, ((1, back_2), (0, back_3))), mid)
    from_1 = swap(join(block_1, share_1, ((1, back_1),)), near)
    share = join(ext, share_0, ((1, back_0), (2, back_far)), F32)
    return call(add_kernel, (share, from_1, from_2), [((rows, features), BF16)])


def is_cube(mesh):
    return mesh.shape["group"] == 2 and mesh.shape["dev"] == 4 and mesh.shape["pair"] == 2


def solution(mesh):
    in_specs = (
        P(("parts", "group", "dev", "pair"), None),
        P(("parts", "group", "dev", "pair"), None),
        P(("parts", "group", "dev", "pair"), None),
        P(("group", "dev"), None, "pair"),
        P(("group", "dev"), None, "pair"),
        P(("group", "dev"), None, "pair"),
    )
    out_specs = P(("parts", "group", "dev", "pair"), None)

    def shards(*args):
        return (travelling_tokens if is_cube(mesh) else gathered_weights)(*args)

    return jax.shard_map(
        shards, mesh=mesh, in_specs=in_specs, out_specs=out_specs, check_vma=False
    )
```

```python
import functools

import jax
import jax.numpy as jnp
from jax import lax
from jax.experimental import pallas as pl
from jax.experimental.pallas import tpu as pltpu
from jax.sharding import PartitionSpec as P


CHIPS = ("group", "dev")
LANES = 128
VMEM_LIMIT = 12 << 20
F32, BF16 = jnp.float32, jnp.bfloat16
LAG = 725


def partner_2(x, axis, apart):
    return lax.ppermute(x, axis, [(i, i ^ 1 << apart) for i in range(lax.axis_size(axis))])


def expert_block(batch_rows, gate_piece, up_piece, down_piece):
    gate_act = jnp.dot(batch_rows, gate_piece, preferred_element_type=jnp.float32)
    up_act = jnp.dot(batch_rows, up_piece, preferred_element_type=jnp.float32)
    hidden = (jax.nn.silu(gate_act) * up_act).astype(jnp.bfloat16)
    return lax.dot_general(
        hidden, down_piece, (((1,), (1,)), ((), ())), preferred_element_type=jnp.float32
    )


def expert_capacity(rows_dev, top_count, experts):
    return 2 * max(1, 3 * rows_dev * top_count // (4 * experts))


def gathered_weights(tokens, expert_ids, route_scores, w_gate, w_up, w_down):
    rows_dev, features = tokens.shape
    top_count = expert_ids.shape[1]
    dest_count = lax.axis_size(("group", "dev"))
    experts = dest_count // 2
    half_cap = expert_capacity(rows_dev, top_count, experts) // 2
    route_weight = route_scores / jnp.sum(route_scores, axis=1, keepdims=True)
    flat_ids = expert_ids.reshape(-1)
    onehot = (flat_ids[:, None] == jnp.arange(experts, dtype=jnp.int32)[None, :]).astype(jnp.int32)
    before = jnp.cumsum(onehot, axis=0) - onehot
    rank_in = jnp.sum(before * onehot, axis=1)
    target = 2 * flat_ids + rank_in // half_cap
    position = target * half_cap + rank_in % half_cap
    owners = jnp.arange(rows_dev * top_count, dtype=jnp.int32) // top_count
    outgoing = (
        jnp.zeros((dest_count * half_cap, features), jnp.bfloat16).at[position].set(tokens[owners])
    )
    outgoing = outgoing.reshape(dest_count, half_cap, features)
    arrived = lax.all_to_all(outgoing, ("group", "dev"), split_axis=0, concat_axis=0, tiled=True)
    batch_rows = arrived.reshape(dest_count * half_cap, features)
    partner = partner_2((w_gate[0], w_up[0], w_down[0]), "dev", 0)
    gate_half = jnp.concatenate([w_gate[0], partner[0]], axis=1)
    up_half = jnp.concatenate([w_up[0], partner[1]], axis=1)
    down_half = jnp.concatenate([w_down[0], partner[2]], axis=1)
    full_gate, full_up, full_down = (
        lax.all_gather(gate_half, "pair", axis=1, tiled=True),
        lax.all_gather(up_half, "pair", axis=1, tiled=True),
        lax.all_gather(down_half, "pair", axis=1, tiled=True),
    )
    result = expert_block(batch_rows, full_gate, full_up, full_down)
    answer = result.astype(jnp.bfloat16).reshape(dest_count, half_cap, features)
    returned = lax.all_to_all(answer, ("group", "dev"), split_axis=0, concat_axis=0, tiled=True)
    picked = returned.reshape(dest_count * half_cap, features)[position].astype(jnp.float32)
    weighted = picked * route_weight.reshape(-1)[:, None]
    mixed_out = jnp.sum(weighted.reshape(rows_dev, top_count, features), axis=1)
    return mixed_out.astype(jnp.bfloat16)


def swap(x, mask):
    return lax.ppermute(x, CHIPS, [(i, i ^ mask) for i in range(lax.axis_size(CHIPS))])


def iota(shape, dim):
    return lax.broadcasted_iota(jnp.int32, shape, dim)


def expert_of(slot, experts):
    group, half = lax.axis_index("group"), lax.axis_index("dev") // 2
    per_group = experts // lax.axis_size("group")
    group = group if slot == 0 else 1 - group
    return group * per_group + (per_group - 1 - half if slot == 2 else half)


def coefficient(meta, expert, experts):
    lane = iota(meta.shape, 1)
    hit = (lane == expert) | (lane == expert + experts) | (lane == expert + 2 * experts)
    return jnp.sum(jnp.where(hit, meta.astype(F32), 0.0), axis=1, keepdims=True)


def places(coef):
    rows = coef.shape[0]
    chosen = jnp.broadcast_to(jnp.where(coef > 0.0, 1.0, 0.0), (rows, rows))
    here, there = iota((rows, rows), 0), iota((rows, rows), 1)
    chosen_row = jnp.sum(jnp.where(here == there, chosen, 0.0), axis=0, keepdims=True)
    rank_row = jnp.sum(jnp.where(here < there, chosen, 0.0), axis=0, keepdims=True)
    return chosen_row, rank_row


def packed(block, coef, cap):
    rows = coef.shape[0]
    chosen_row, rank_row = places(coef)
    slot = iota((cap, rows), 0).astype(F32)
    select = jnp.where((slot == rank_row) & (chosen_row > 0.0), 1.0, 0.0).astype(BF16)
    return jnp.dot(select, block, preferred_element_type=F32).astype(BF16)


def unpacked(part, coef):
    rows, cap = coef.shape[0], part.shape[0]
    chosen_row, _ = places(coef)
    here, there = iota((rows, rows), 0), iota((rows, rows), 1)
    rank = jnp.sum(jnp.where(there < here, chosen_row, 0.0), axis=1, keepdims=True)
    slot = iota((rows, cap), 1).astype(F32)
    select = jnp.where((slot == rank) & (coef > 0.0), 1.0, 0.0).astype(BF16)
    return coef * jnp.dot(select, part, preferred_element_type=F32)


def column(row, rows):
    same = iota((rows, rows), 0) == iota((rows, rows), 1)
    return jnp.sum(jnp.where(same, jnp.broadcast_to(row, (rows, rows)), 0.0), axis=1, keepdims=True)


def prepare_kernel(experts, tokens, ids, scores, ext, ids_here, scores_here, count, sems):
    rows, features = tokens.shape
    copies = [
        pltpu.make_async_copy(ids, ids_here, sems.at[0]),
        pltpu.make_async_copy(scores, scores_here, sems.at[1]),
        pltpu.make_async_copy(tokens, ext.at[:, :features], sems.at[2]),
    ]
    for copy in copies:
        copy.start()
    copies[0].wait()
    copies[1].wait()
    weight = scores_here[...] / jnp.sum(scores_here[...], axis=0, keepdims=True)
    lane = iota((rows, LANES), 1).astype(F32)
    meta = jnp.zeros((rows, LANES), F32)
    for k in range(ids.shape[0]):
        chosen = column(ids_here[k : k + 1, :].astype(F32), rows)
        rest = column(weight[k : k + 1, :], rows)
        for part in range(3):
            term = rest.astype(BF16).astype(F32)
            meta += jnp.where(lane == chosen + float(part * experts), term, 0.0)
            rest = rest - term
    ext[:, features:] = meta.astype(BF16)
    copies[2].wait()
    count[0] = 0

    @pl.loop(0, LAG * lax.axis_index("pair"))
    def _(i):
        count[0] = count[0] * 3 + i


def pack_kernel(experts, slots, block, *outs):
    features = outs[0].shape[1]
    for slot, out in zip(slots, outs):
        coef = coefficient(block[:, features:], expert_of(slot, experts), experts)
        out[...] = packed(block[:, :features], coef, out.shape[0])


def hold_kernel(experts, slots, block, *refs):
    sems, outs = refs[-1], refs[-1 - len(slots) : -1]
    half = (len(refs) - len(outs)) // 2
    copies = [
        pltpu.make_async_copy(src, dst, sems.at[i])
        for i, (src, dst) in enumerate(zip(refs[:half], refs[half : 2 * half]))
    ]
    for copy in copies:
        copy.start()
    pack_kernel(experts, slots, block, *outs)
    for copy in copies:
        copy.wait()


def expert_kernel(experts, whole, packs, *refs):
    weights, blocks = refs[:6], refs[6 : 6 + whole + packs]
    outs = refs[6 + whole + packs :]
    features = outs[0].shape[1]
    rows = jnp.concatenate([b[:, :features] for b in blocks], axis=0)
    total = None
    for gate, up, down in (weights[:3], weights[3:]):
        across = (((1,), (1,)), ((), ()))
        gate_act = lax.dot_general(rows, gate[...], across, preferred_element_type=F32)
        up_act = lax.dot_general(rows, up[...], across, preferred_element_type=F32)
        hidden = (gate_act / (1.0 + jnp.exp(-gate_act)) * up_act).astype(BF16)
        part = jnp.dot(hidden, down[...], preferred_element_type=F32)
        total = part if total is None else total + part
    at = 0
    for i, (block, out) in enumerate(zip(blocks, outs)):
        part = total[at : at + block.shape[0]]
        if i < whole:
            part = part * coefficient(block[:, features:], expert_of(0, experts), experts)
        out[...] = part.astype(out.dtype)
        at += block.shape[0]


def join_kernel(experts, slots, block, share, *refs):
    out, features = refs[-1], share.shape[1]
    total = share[...].astype(F32)
    for slot, back in zip(slots, refs[:-1]):
        coef = coefficient(block[:, features:], expert_of(slot, experts), experts)
        total += unpacked(back[...], coef)
    out[...] = total.astype(out.dtype)


def add_kernel(share, one, two, out, here, sems):
    parts = sems.shape[0]
    rows = share.shape[0] // parts
    copies = []
    for i in range(parts):
        at = pl.ds(i * rows, rows)
        here[at] = (share[at] + one[at].astype(F32) + two[at].astype(F32)).astype(here.dtype)
        copies.append(pltpu.make_async_copy(here.at[at], out.at[at], sems.at[i]))
        copies[-1].start()
    for copy in copies:
        copy.wait()


def call(kernel, operands, outs, flops=0, far_operands=0, scratch=(), space=pltpu.VMEM):
    shapes = [jax.ShapeDtypeStruct(s, d) for s, d in outs]
    moved = sum(a.size * a.dtype.itemsize for a in (*operands, *shapes))
    spaces = [pltpu.VMEM] * (len(operands) - far_operands) + [pltpu.HBM] * far_operands
    operands = [
        pltpu.with_memory_space_constraint(a, m) if m is pltpu.HBM else a
        for a, m in zip(operands, spaces)
    ]
    result = pl.pallas_call(
        kernel,
        out_shape=shapes,
        in_specs=[pl.BlockSpec(memory_space=m) for m in spaces],
        out_specs=[pl.BlockSpec(memory_space=space)] * len(shapes),
        scratch_shapes=scratch,
        compiler_params=pltpu.CompilerParams(vmem_limit_bytes=VMEM_LIMIT),
        cost_estimate=pl.CostEstimate(flops=flops, bytes_accessed=moved, transcendentals=0),
    )(*operands)
    return result[0] if len(shapes) == 1 else result


def travelling_tokens(tokens, expert_ids, route_scores, w_gate, w_up, w_down):
    rows, features = tokens.shape
    top = expert_ids.shape[1]
    devs = lax.axis_size("dev")
    experts = lax.axis_size(CHIPS) // 2
    cap = min(rows, expert_capacity(rows, top, experts))
    near, mid, cross = 1, devs // 2, devs
    width = features + LANES

    mine = tuple(w[0].T for w in (w_gate, w_up, w_down))
    pair = lax.axis_size("pair")
    theirs = []
    for w in mine:
        theirs.append(lax.ppermute(w, "pair", [(i, pair - 1 - i) for i in range(pair)]))
    per_row = 2 * 3 * 2 * mine[0].shape[0] * features

    def compute(blocks, outs):
        whole = sum(b.shape[1] == width for b in blocks)
        kernel = functools.partial(expert_kernel, experts, whole, len(blocks) - whole)
        sizes = [b.shape[0] for b in blocks]
        shapes = [((n, features), d) for n, d in zip(sizes, outs)]
        return call(kernel, weights + tuple(blocks), shapes, per_row * sum(sizes))

    def join(block, share, backs, dtype=BF16):
        kernel = functools.partial(join_kernel, experts, tuple(slot for slot, _ in backs))
        operands = (block, share) + tuple(back for _, back in backs)
        return call(kernel, operands, [((rows, features), dtype)], 2 * rows * cap * features)

    def pack(block, *slots):
        kernel = functools.partial(pack_kernel, experts, slots)
        flops = 2 * len(slots) * cap * rows * features
        return call(kernel, (block,), [packed_out] * len(slots), flops)

    packed_out = ((cap, features), BF16)
    scratch = [pltpu.VMEM((top, rows), jnp.int32), pltpu.VMEM((top, rows), F32)]
    scratch += [pltpu.SMEM((1,), jnp.int32), pltpu.SemaphoreType.DMA((3,))]
    sources = (tokens, expert_ids.T, route_scores.T)
    kernel = functools.partial(prepare_kernel, experts)
    ext = call(kernel, sources, [((rows, width), BF16)], 0, len(sources), scratch)
    kernel = functools.partial(hold_kernel, experts, (1, 2))
    shapes = [(w.shape, w.dtype) for w in mine] + [packed_out] * 2
    sems = [pltpu.SemaphoreType.DMA((len(mine),))]
    *held, side_0, far_0 = call(kernel, (ext,) + mine, shapes, 0, len(mine), sems)
    weights = tuple(held) + tuple(theirs)
    block_2 = swap(ext, mid)
    block_1 = swap(ext, near)
    rows_0 = swap(side_0, cross)
    pass_3, side_2 = pack(block_2, 0, 1)
    side_1 = pack(block_1, 1)
    rows_3 = swap(pass_3, near)
    rows_2 = swap(side_2, cross)
    rows_1 = swap(side_1, cross)
    rows_far = swap(far_0, cross + mid + near)

    share_0, share_1, share_2, back_0 = compute(
        (ext, block_1, block_2, rows_0), (F32, F32, F32, BF16)
    )
    back_3, back_2 = compute((rows_3, rows_2), (BF16, BF16))
    back_1, back_far = compute((rows_1, rows_far), (BF16, BF16))

    back_3 = swap(back_3, near)
    back_2 = swap(back_2, cross)
    back_1 = swap(back_1, cross)
    back_far = swap(back_far, cross + mid + near)
    back_0 = swap(back_0, cross)
    from_2 = swap(join(block_2, share_2, ((1, back_2), (0, back_3))), mid)
    from_1 = swap(join(block_1, share_1, ((1, back_1),)), near)
    share = join(ext, share_0, ((1, back_0), (2, back_far)), F32)
    scratch = [pltpu.VMEM((rows, features), BF16), pltpu.SemaphoreType.DMA((4,))]
    mixed = [((rows, features), BF16)]
    return call(add_kernel, (share, from_1, from_2), mixed, 0, 0, scratch, pltpu.HBM)


def is_cube(mesh):
    return mesh.shape["group"] == 2 and mesh.shape["dev"] == 4 and mesh.shape["pair"] == 2


def solution(mesh):
    in_specs = (
        P(("parts", "group", "dev", "pair"), None),
        P(("parts", "group", "dev", "pair"), None),
        P(("parts", "group", "dev", "pair"), None),
        P(("group", "dev"), None, "pair"),
        P(("group", "dev"), None, "pair"),
        P(("group", "dev"), None, "pair"),
    )
    out_specs = P(("parts", "group", "dev", "pair"), None)

    def shards(*args):
        return (travelling_tokens if is_cube(mesh) else gathered_weights)(*args)

    return jax.shard_map(
        shards, mesh=mesh, in_specs=in_specs, out_specs=out_specs, check_vma=False
    )
```

```python
import functools

import jax
import jax.numpy as jnp
from jax import lax
from jax.experimental import pallas as pl
from jax.experimental.pallas import tpu as pltpu
from jax.sharding import PartitionSpec as P


CHIPS = ("group", "dev")
LANES = 128
VMEM_LIMIT = 12 << 20
F32, BF16 = jnp.float32, jnp.bfloat16
LAG = 690


def partner_2(x, axis, apart):
    return lax.ppermute(x, axis, [(i, i ^ 1 << apart) for i in range(lax.axis_size(axis))])


def expert_block(batch_rows, gate_piece, up_piece, down_piece):
    gate_act = jnp.dot(batch_rows, gate_piece, preferred_element_type=jnp.float32)
    up_act = jnp.dot(batch_rows, up_piece, preferred_element_type=jnp.float32)
    hidden = (jax.nn.silu(gate_act) * up_act).astype(jnp.bfloat16)
    return lax.dot_general(
        hidden, down_piece, (((1,), (1,)), ((), ())), preferred_element_type=jnp.float32
    )


def expert_capacity(rows_dev, top_count, experts):
    return 2 * max(1, 3 * rows_dev * top_count // (4 * experts))


def gathered_weights(tokens, expert_ids, route_scores, w_gate, w_up, w_down):
    rows_dev, features = tokens.shape
    top_count = expert_ids.shape[1]
    dest_count = lax.axis_size(("group", "dev"))
    experts = dest_count // 2
    half_cap = expert_capacity(rows_dev, top_count, experts) // 2
    route_weight = route_scores / jnp.sum(route_scores, axis=1, keepdims=True)
    flat_ids = expert_ids.reshape(-1)
    onehot = (flat_ids[:, None] == jnp.arange(experts, dtype=jnp.int32)[None, :]).astype(jnp.int32)
    before = jnp.cumsum(onehot, axis=0) - onehot
    rank_in = jnp.sum(before * onehot, axis=1)
    target = 2 * flat_ids + rank_in // half_cap
    position = target * half_cap + rank_in % half_cap
    owners = jnp.arange(rows_dev * top_count, dtype=jnp.int32) // top_count
    outgoing = (
        jnp.zeros((dest_count * half_cap, features), jnp.bfloat16).at[position].set(tokens[owners])
    )
    outgoing = outgoing.reshape(dest_count, half_cap, features)
    arrived = lax.all_to_all(outgoing, ("group", "dev"), split_axis=0, concat_axis=0, tiled=True)
    batch_rows = arrived.reshape(dest_count * half_cap, features)
    partner = partner_2((w_gate[0], w_up[0], w_down[0]), "dev", 0)
    gate_half = jnp.concatenate([w_gate[0], partner[0]], axis=1)
    up_half = jnp.concatenate([w_up[0], partner[1]], axis=1)
    down_half = jnp.concatenate([w_down[0], partner[2]], axis=1)
    full_gate, full_up, full_down = (
        lax.all_gather(gate_half, "pair", axis=1, tiled=True),
        lax.all_gather(up_half, "pair", axis=1, tiled=True),
        lax.all_gather(down_half, "pair", axis=1, tiled=True),
    )
    result = expert_block(batch_rows, full_gate, full_up, full_down)
    answer = result.astype(jnp.bfloat16).reshape(dest_count, half_cap, features)
    returned = lax.all_to_all(answer, ("group", "dev"), split_axis=0, concat_axis=0, tiled=True)
    picked = returned.reshape(dest_count * half_cap, features)[position].astype(jnp.float32)
    weighted = picked * route_weight.reshape(-1)[:, None]
    mixed_out = jnp.sum(weighted.reshape(rows_dev, top_count, features), axis=1)
    return mixed_out.astype(jnp.bfloat16)


def swap(x, mask):
    return lax.ppermute(x, CHIPS, [(i, i ^ mask) for i in range(lax.axis_size(CHIPS))])


def iota(shape, dim):
    return lax.broadcasted_iota(jnp.int32, shape, dim)


def expert_of(slot, experts):
    group, half = lax.axis_index("group"), lax.axis_index("dev") // 2
    per_group = experts // lax.axis_size("group")
    group = group if slot == 0 else 1 - group
    return group * per_group + (per_group - 1 - half if slot == 2 else half)


def coefficient(meta, expert, experts):
    lane = iota(meta.shape, 1)
    hit = (lane == expert) | (lane == expert + experts) | (lane == expert + 2 * experts)
    return jnp.sum(jnp.where(hit, meta.astype(F32), 0.0), axis=1, keepdims=True)


def places(coef):
    rows = coef.shape[0]
    chosen = jnp.broadcast_to(jnp.where(coef > 0.0, 1.0, 0.0), (rows, rows))
    here, there = iota((rows, rows), 0), iota((rows, rows), 1)
    chosen_row = jnp.sum(jnp.where(here == there, chosen, 0.0), axis=0, keepdims=True)
    rank_row = jnp.sum(jnp.where(here < there, chosen, 0.0), axis=0, keepdims=True)
    return chosen_row, rank_row


def packed(block, coef, cap):
    rows = coef.shape[0]
    chosen_row, rank_row = places(coef)
    slot = iota((cap, rows), 0).astype(F32)
    select = jnp.where((slot == rank_row) & (chosen_row > 0.0), 1.0, 0.0).astype(BF16)
    return jnp.dot(select, block, preferred_element_type=F32).astype(BF16)


def unpacked(part, coef):
    rows, cap = coef.shape[0], part.shape[0]
    chosen_row, _ = places(coef)
    here, there = iota((rows, rows), 0), iota((rows, rows), 1)
    rank = jnp.sum(jnp.where(there < here, chosen_row, 0.0), axis=1, keepdims=True)
    slot = iota((rows, cap), 1).astype(F32)
    select = jnp.where((slot == rank) & (coef > 0.0), 1.0, 0.0).astype(BF16)
    return coef * jnp.dot(select, part, preferred_element_type=F32)


def column(row, rows):
    same = iota((rows, rows), 0) == iota((rows, rows), 1)
    return jnp.sum(jnp.where(same, jnp.broadcast_to(row, (rows, rows)), 0.0), axis=1, keepdims=True)


def prepare_kernel(experts, tokens, ids, scores, ext, ids_here, scores_here, count, sems):
    rows, features = tokens.shape
    copies = [
        pltpu.make_async_copy(ids, ids_here, sems.at[0]),
        pltpu.make_async_copy(scores, scores_here, sems.at[1]),
        pltpu.make_async_copy(tokens, ext.at[:, :features], sems.at[2]),
    ]
    for copy in copies:
        copy.start()
    copies[0].wait()
    copies[1].wait()
    weight = scores_here[...] / jnp.sum(scores_here[...], axis=0, keepdims=True)
    lane = iota((rows, LANES), 1).astype(F32)
    meta = jnp.zeros((rows, LANES), F32)
    for k in range(ids.shape[0]):
        chosen = column(ids_here[k : k + 1, :].astype(F32), rows)
        rest = column(weight[k : k + 1, :], rows)
        for part in range(3):
            term = rest.astype(BF16).astype(F32)
            meta += jnp.where(lane == chosen + float(part * experts), term, 0.0)
            rest = rest - term
    ext[:, features:] = meta.astype(BF16)
    copies[2].wait()
    count[0] = 0

    @pl.loop(0, LAG * lax.axis_index("pair"))
    def _(i):
        count[0] = count[0] * 3 + i


def pack_kernel(experts, slots, block, *outs):
    features = outs[0].shape[1]
    for slot, out in zip(slots, outs):
        coef = coefficient(block[:, features:], expert_of(slot, experts), experts)
        out[...] = packed(block[:, :features], coef, out.shape[0])


def hold_kernel(experts, slots, block, *refs):
    sems, outs = refs[-1], refs[-1 - len(slots) : -1]
    half = (len(refs) - len(outs)) // 2
    copies = [
        pltpu.make_async_copy(src, dst, sems.at[i])
        for i, (src, dst) in enumerate(zip(refs[:half], refs[half : 2 * half]))
    ]
    for copy in copies:
        copy.start()
    pack_kernel(experts, slots, block, *outs)
    for copy in copies:
        copy.wait()


def expert_kernel(experts, whole, packs, *refs):
    weights, blocks = refs[:6], refs[6 : 6 + whole + packs]
    outs = refs[6 + whole + packs :]
    features = outs[0].shape[1]
    rows = jnp.concatenate([b[:, :features] for b in blocks], axis=0)
    total = None
    for gate, up, down in (weights[:3], weights[3:]):
        across = (((1,), (1,)), ((), ()))
        gate_act = lax.dot_general(rows, gate[...], across, preferred_element_type=F32)
        up_act = lax.dot_general(rows, up[...], across, preferred_element_type=F32)
        hidden = (gate_act / (1.0 + jnp.exp(-gate_act)) * up_act).astype(BF16)
        part = jnp.dot(hidden, down[...], preferred_element_type=F32)
        total = part if total is None else total + part
    at = 0
    for i, (block, out) in enumerate(zip(blocks, outs)):
        part = total[at : at + block.shape[0]]
        if i < whole:
            part = part * coefficient(block[:, features:], expert_of(0, experts), experts)
        out[...] = part.astype(out.dtype)
        at += block.shape[0]


def join_kernel(experts, slots, block, share, *refs):
    out, features = refs[-1], share.shape[1]
    total = share[...].astype(F32)
    for slot, back in zip(slots, refs[:-1]):
        coef = coefficient(block[:, features:], expert_of(slot, experts), experts)
        total += unpacked(back[...], coef)
    out[...] = total.astype(out.dtype)


def add_kernel(share, one, two, out, here, sems):
    parts = sems.shape[0]
    rows = share.shape[0] // parts
    copies = []
    for i in range(parts):
        at = pl.ds(i * rows, rows)
        here[at] = (share[at] + one[at].astype(F32) + two[at].astype(F32)).astype(here.dtype)
        copies.append(pltpu.make_async_copy(here.at[at], out.at[at], sems.at[i]))
        copies[-1].start()
    for copy in copies:
        copy.wait()


def call(kernel, operands, outs, flops=0, far_operands=0, scratch=(), space=pltpu.VMEM):
    shapes = [jax.ShapeDtypeStruct(s, d) for s, d in outs]
    moved = sum(a.size * a.dtype.itemsize for a in (*operands, *shapes))
    spaces = [pltpu.VMEM] * (len(operands) - far_operands) + [pltpu.HBM] * far_operands
    operands = [
        pltpu.with_memory_space_constraint(a, m) if m is pltpu.HBM else a
        for a, m in zip(operands, spaces)
    ]
    result = pl.pallas_call(
        kernel,
        out_shape=shapes,
        in_specs=[pl.BlockSpec(memory_space=m) for m in spaces],
        out_specs=[pl.BlockSpec(memory_space=space)] * len(shapes),
        scratch_shapes=scratch,
        compiler_params=pltpu.CompilerParams(vmem_limit_bytes=VMEM_LIMIT),
        cost_estimate=pl.CostEstimate(flops=flops, bytes_accessed=moved, transcendentals=0),
    )(*operands)
    return result[0] if len(shapes) == 1 else result


def travelling_tokens(tokens, expert_ids, route_scores, w_gate, w_up, w_down):
    rows, features = tokens.shape
    top = expert_ids.shape[1]
    devs = lax.axis_size("dev")
    experts = lax.axis_size(CHIPS) // 2
    cap = min(rows, expert_capacity(rows, top, experts))
    near, mid, cross = 1, devs // 2, devs
    width = features + LANES

    mine = tuple(w[0].T for w in (w_gate, w_up, w_down))
    pair = lax.axis_size("pair")
    theirs = []
    for w in mine:
        theirs.append(lax.ppermute(w, "pair", [(i, pair - 1 - i) for i in range(pair)]))
    per_row = 2 * 3 * 2 * mine[0].shape[0] * features

    def compute(blocks, outs):
        whole = sum(b.shape[1] == width for b in blocks)
        kernel = functools.partial(expert_kernel, experts, whole, len(blocks) - whole)
        sizes = [b.shape[0] for b in blocks]
        shapes = [((n, features), d) for n, d in zip(sizes, outs)]
        return call(kernel, weights + tuple(blocks), shapes, per_row * sum(sizes))

    def join(block, share, backs, dtype=BF16):
        kernel = functools.partial(join_kernel, experts, tuple(slot for slot, _ in backs))
        operands = (block, share) + tuple(back for _, back in backs)
        return call(kernel, operands, [((rows, features), dtype)], 2 * rows * cap * features)

    def pack(block, *slots):
        kernel = functools.partial(pack_kernel, experts, slots)
        flops = 2 * len(slots) * cap * rows * features
        return call(kernel, (block,), [packed_out] * len(slots), flops)

    packed_out = ((cap, features), BF16)
    scratch = [pltpu.VMEM((top, rows), jnp.int32), pltpu.VMEM((top, rows), F32)]
    scratch += [pltpu.SMEM((1,), jnp.int32), pltpu.SemaphoreType.DMA((3,))]
    sources = (tokens, expert_ids.T, route_scores.T)
    kernel = functools.partial(prepare_kernel, experts)
    ext = call(kernel, sources, [((rows, width), BF16)], 0, len(sources), scratch)
    kernel = functools.partial(hold_kernel, experts, (1, 2))
    shapes = [(w.shape, w.dtype) for w in mine] + [packed_out] * 2
    sems = [pltpu.SemaphoreType.DMA((len(mine),))]
    *held, side_0, far_0 = call(kernel, (ext,) + mine, shapes, 0, len(mine), sems)
    weights = tuple(held) + tuple(theirs)
    block_2 = swap(ext, mid)
    block_1 = swap(ext, near)
    rows_0 = swap(side_0, cross)
    pass_3, side_2 = pack(block_2, 0, 1)
    side_1 = pack(block_1, 1)
    rows_3 = swap(pass_3, near)
    rows_2 = swap(side_2, cross)
    rows_1 = swap(side_1, cross)
    rows_far = swap(far_0, cross + mid + near)

    share_0, share_1, share_2, back_0 = compute(
        (ext, block_1, block_2, rows_0), (F32, F32, F32, BF16)
    )
    back_3, back_2 = compute((rows_3, rows_2), (BF16, BF16))
    back_1, back_far = compute((rows_1, rows_far), (BF16, BF16))

    back_3 = swap(back_3, near)
    back_2 = swap(back_2, cross)
    back_1 = swap(back_1, cross)
    back_far = swap(back_far, cross + near)
    back_0 = swap(back_0, cross)
    from_2 = swap(join(block_2, share_2, ((1, back_2), (1, back_far), (0, back_3))), mid)
    from_1 = swap(join(block_1, share_1, ((1, back_1),)), near)
    share = join(ext, share_0, ((1, back_0),), F32)
    scratch = [pltpu.VMEM((rows, features), BF16), pltpu.SemaphoreType.DMA((4,))]
    mixed = [((rows, features), BF16)]
    return call(add_kernel, (share, from_1, from_2), mixed, 0, 0, scratch, pltpu.HBM)


def is_cube(mesh):
    return mesh.shape["group"] == 2 and mesh.shape["dev"] == 4 and mesh.shape["pair"] == 2


def solution(mesh):
    in_specs = (
        P(("parts", "group", "dev", "pair"), None),
        P(("parts", "group", "dev", "pair"), None),
        P(("parts", "group", "dev", "pair"), None),
        P(("group", "dev"), None, "pair"),
        P(("group", "dev"), None, "pair"),
        P(("group", "dev"), None, "pair"),
    )
    out_specs = P(("parts", "group", "dev", "pair"), None)

    def shards(*args):
        return (travelling_tokens if is_cube(mesh) else gathered_weights)(*args)

    return jax.shard_map(
        shards, mesh=mesh, in_specs=in_specs, out_specs=out_specs, check_vma=False
    )
```
